128 devices in a mesh: freq: 16 (over z, y_lo, core), cell: 8 (over y_hi, x).
Axes of the slice: x: 4, y: 4 (y_hi: 2, y_lo: 2; y = y_hi * 2 + y_lo), z: 4, core: 2. Of those that a mesh axis runs over, the one named last changes fastest.
Arguments:
- covariance: bfloat16 [512, 2, 256, 256], P('freq', None, 'cell'), may hold values from -4 to 6, as said below
- replica: bfloat16 [512, 2, 256, 4096], P('freq', None, None, 'cell'), may hold values from -0.25 to 0.25
- transmission: bfloat16 [512, 4096], P('freq', 'cell'), may hold values from 0.29882812 to 3
Outputs:
- ambiguity: float32 [4096], P('cell')
- relative: float32 [4096], P('cell')
The draws below stay inside these ranges and needn't reach their ends.
Inputs may be any that keep to these rules, and one draw needn't show every extreme that they name: Each covariance[f, 0] + i covariance[f, 1] is exactly Hermitian, also after rounding to bfloat16; before rounding all its eigenvalues are at least 0.5.
All inputs are finite; a program needn't handle non-finite values.
Results may differ from the reference program's by a relative error of at most 0.0003.
Values may be sent and summed in bfloat16 or wider, within the bound.
A program may use at most 384 MiB of HBM per device.

```python
import math
import jax
import jax.numpy as jnp
from jax import lax

NR = 256
FREQS = 512
CELLS = 4096


def drawn(key):
    count = 3
    key_cells, key_source = jax.random.split(jax.random.fold_in(key, 41))
    span = CELLS // count
    cells = jax.random.randint(key_cells, (count,), 0, span, dtype=jnp.int32) + span * jnp.arange(count, dtype=jnp.int32)
    bound = 0.25 * (2.0 * NR) ** 0.5
    source = jax.random.truncated_normal(key_source, -bound, bound, (FREQS, 2, NR, count), jnp.float32) / (2.0 * NR) ** 0.5
    return (cells, source)


def draw_replica(key, part):
    cells, source = drawn(key)
    bound = 0.25 * (2.0 * NR) ** 0.5
    field = jax.random.truncated_normal(jax.random.fold_in(key, 43), -bound, bound, (FREQS, 2, NR, CELLS), jnp.float32) / (2.0 * NR) ** 0.5
    position = jnp.arange(CELLS, dtype=jnp.int32)
    for index in range(source.shape[3]):
        field = jnp.where(position == cells[index], source[:, :, :, index:index + 1], field)
    return field.astype(jnp.bfloat16)


def draw_covariance(key, part):
    cells, source = drawn(key)
    key_re, key_im = jax.random.split(jax.random.fold_in(key, 17), 2)
    key_power = jax.random.fold_in(key, 29)
    real = jax.random.normal(key_re, (FREQS, NR, NR), jnp.float32)
    imag = jax.random.normal(key_im, (FREQS, NR, NR), jnp.float32)
    count = source.shape[3]
    powers = jnp.exp(jax.random.uniform(key_power, (FREQS, count), jnp.float32, jnp.log(6.0), jnp.log(30.0)))
    scale = 1.0 / (2.0 * NR)
    gram_re = (jnp.einsum('fik,fjk->fij', real, real, precision=lax.Precision.HIGHEST) + jnp.einsum('fik,fjk->fij', imag, imag, precision=lax.Precision.HIGHEST)) * scale
    gram_im = (jnp.einsum('fik,fjk->fij', imag, real, precision=lax.Precision.HIGHEST) - jnp.einsum('fik,fjk->fij', real, imag, precision=lax.Precision.HIGHEST)) * scale
    part_re = source[:, 0]
    part_im = source[:, 1]
    weighted_re = part_re * powers[:, None, :]
    weighted_im = part_im * powers[:, None, :]
    signal_re = jnp.einsum('fik,fjk->fij', weighted_re, part_re, precision=lax.Precision.HIGHEST) + jnp.einsum('fik,fjk->fij', weighted_im, part_im, precision=lax.Precision.HIGHEST)
    signal_im = jnp.einsum('fik,fjk->fij', weighted_im, part_re, precision=lax.Precision.HIGHEST) - jnp.einsum('fik,fjk->fij', weighted_re, part_im, precision=lax.Precision.HIGHEST)
    mixed_re = gram_re + signal_re
    mixed_im = gram_im + signal_im
    cov_re = 0.5 * (mixed_re + jnp.swapaxes(mixed_re, 1, 2)) + 0.5 * jnp.eye(NR, dtype=jnp.float32)
    cov_im = 0.5 * (mixed_im - jnp.swapaxes(mixed_im, 1, 2))
    cov_re = jnp.clip(cov_re, -4.0, 6.0)
    cov_im = jnp.clip(cov_im, -4.0, 4.0)
    return jnp.stack([cov_re, cov_im], axis=1).astype(jnp.bfloat16)


def block_scale(own_key, dims, shards, smallest, high):
    factor_of, own = 1.0, jax.random.fold_in(own_key, 6)
    for axis_at, shards_of in shards:
        steps = jnp.exp(jax.random.uniform(jax.random.fold_in(own, axis_at), (shards_of,), jnp.float32, smallest / len(shards), high / len(shards)))
        factor_of = factor_of * jnp.repeat(steps, dims[axis_at] // shards_of).reshape([-1 if axis == axis_at else 1 for axis in range(len(dims))])
    return factor_of


def setup_inputs(seed: int = 0) -> dict:
    key_of = jax.random.split(jax.random.key(seed), 4)
    return {
        "covariance": draw_covariance(jax.random.fold_in(key_of[3], 71), 0),
        "replica": draw_replica(jax.random.fold_in(key_of[3], 71), 0),
        "transmission": jnp.clip(jnp.exp(math.log(3.0) - 2.306499 * jax.random.uniform(key_of[2], (FREQS, CELLS), jnp.float32) ** block_scale(key_of[2], (FREQS, CELLS), ((0, 16), (1, 8)), -0.2, 0.2)), 0.29882812, 3.0).astype(jnp.bfloat16),
    }


def one_frequency(items):
    cov_f, rep_f, trans_f = items
    stacked = cov_f.reshape(2 * NR, NR)
    first = jnp.dot(stacked, rep_f[0], preferred_element_type=jnp.float32)
    second = jnp.dot(stacked, rep_f[1], preferred_element_type=jnp.float32)
    image_re = first[:NR] - second[NR:]
    image_im = first[NR:] + second[:NR]
    power = jnp.sum(rep_f[0].astype(jnp.float32) * image_re + rep_f[1].astype(jnp.float32) * image_im, axis=0)
    amplitude = trans_f.astype(jnp.float32)
    return amplitude * amplitude * power


def reference(covariance, replica, transmission):
    powers = lax.map(one_frequency, (covariance, replica, transmission))
    ambiguity = jnp.sum(powers, axis=0) / jnp.float32(FREQS)
    peak = jnp.max(ambiguity)
    relative = ambiguity / jnp.maximum(peak, jnp.float32(1.0))
    return ambiguity, relative
```

```python
import functools

import jax
import jax.numpy as jnp
from jax import lax
from jax.experimental import pallas as pl
from jax.experimental.pallas import tpu as pltpu
from jax.sharding import PartitionSpec as P

MESH = pl.DeviceIdType.MESH
CHUNKS = ((4, "x"), (4, "y"), (4, "x"), (4, "y"), (4, "x"), (4, "y"), (4, "x"), (4, "x"))
AHEAD = 2
KINDS = 9


def kernel(
    cov_hbm, rep_hbm, trans_hbm, out_ref,
    diag, gathered, field, trans, weight, matrix, acc, sums, peaks,
    load_sem, rep_sem, send_sem, recv_sem, sum_send, sum_recv, peak_send, peak_recv,
):
    freq, cell = lax.axis_index("freq"), lax.axis_index("cell")
    n_freq, n_cell = lax.axis_size("freq"), lax.axis_size("cell")
    ring = n_cell // 2
    x, row = lax.rem(cell, ring), lax.div(cell, ring)

    def at(shift, other=False):
        r = 1 - row if other else row
        return r * ring + lax.rem(x + shift + ring, ring)

    lanes = gathered.shape[-1]
    own = pl.ds(pl.multiple_of(row * lanes, lanes), lanes)
    far = pl.ds(pl.multiple_of((1 - row) * lanes, lanes), lanes)
    diag_load = pltpu.make_async_copy(cov_hbm.at[:, :, :, own], diag, load_sem.at[0])
    far_load = pltpu.make_async_copy(
        cov_hbm.at[:, row, :, far], gathered.at[cell, :, 1], load_sem.at[1]
    )
    trans_load = pltpu.make_async_copy(trans_hbm, trans, load_sem.at[2])
    diag_load.start()
    far_load.start()
    trans_load.start()
    starts = [sum(c[0] for c in CHUNKS[:i]) for i in range(len(CHUNKS))]
    loads = []
    for i, (size, _) in enumerate(CHUNKS):
        part = pl.ds(starts[i], size)
        loads.append(pltpu.make_async_copy(rep_hbm.at[part], field.at[part], rep_sem.at[i]))
        loads[-1].start()

    barrier = pltpu.get_barrier_semaphore()
    for step in range(1, n_freq):
        pl.semaphore_signal(
            barrier, inc=1, device_id={"freq": lax.rem(freq + step, n_freq)}, device_id_type=MESH
        )
    for step in range(1, n_cell):
        pl.semaphore_signal(
            barrier, inc=1, device_id={"cell": lax.rem(cell + step, n_cell)}, device_id_type=MESH
        )

    diag_load.wait()
    shape = diag.shape[2:]
    line = lax.broadcasted_iota(jnp.int32, shape, 0) + x * shape[0]
    column = lax.broadcasted_iota(jnp.int32, shape, 1)
    factor = jnp.where(line == column, 0.5, 1.0).astype(jnp.float32)
    above = line <= column

    def pack(f, carry):
        re = diag[f, 0].astype(jnp.float32) * factor
        im = diag[f, 1].astype(jnp.float32)
        gathered[cell, f, 0] = jnp.where(above, re, im).astype(jnp.bfloat16)
        return carry

    lax.fori_loop(0, diag.shape[0], pack, 0, unroll=4)
    trans_load.wait()
    amplitude = trans[...].astype(jnp.float32)
    weight[...] = amplitude * amplitude
    acc[...] = jnp.zeros_like(acc)
    far_load.wait()
    pl.semaphore_wait(barrier, n_freq + n_cell - 2)

    def send(chunk, kind, piece, target, half=None):
        size = CHUNKS[chunk][0]
        first = starts[chunk]
        if half is not None:
            size //= 2
            first += half * size
        ref = gathered.at[piece, pl.ds(first, size)]
        copy = pltpu.make_async_remote_copy(
            src_ref=ref, dst_ref=ref,
            send_sem=send_sem.at[chunk, kind], recv_sem=recv_sem.at[chunk, kind],
            device_id={"cell": target}, device_id_type=MESH,
        )
        copy.start()
        return copy

    right, left, partner = at(1), at(-1), at(0, True)
    chunks = len(CHUNKS)
    zero = [None] * chunks
    one = [None] * chunks
    two = [None] * chunks

    def issue_zero(c):
        zero[c] = (
            send(c, 2, cell, partner), send(c, 0, cell, right), send(c, 1, cell, left),
        )

    def issue_one(c):
        to_partner, to_right, to_left = zero[c]
        if CHUNKS[c][1] == "x":
            to_right.wait_recv()
            a = send(c, 5, left, right, 0)
            to_left.wait_recv()
            b = send(c, 6, right, left, 1)
            to_partner.wait_recv()
            one[c] = (a, b, send(c, 3, partner, right), send(c, 4, partner, left))
        else:
            to_right.wait_recv()
            a = send(c, 5, left, right, 0)
            d = send(c, 3, left, partner)
            to_left.wait_recv()
            b = send(c, 6, right, left, 1)
            e = send(c, 4, right, partner)
            to_partner.wait_recv()
            one[c] = (a, b, d, e)

    def issue_two(c):
        a, b, d, e = one[c]
        if CHUNKS[c][1] == "x":
            d.wait_recv()
            g = send(c, 7, at(-1, True), right, 0)
            e.wait_recv()
            h = send(c, 8, at(1, True), left, 1)
            a.wait_recv()
            b.wait_recv()
            two[c] = (g, h)
        else:
            a.wait_recv()
            b.wait_recv()
            two[c] = (send(c, 7, at(2), partner),)
            d.wait_recv()
            e.wait_recv()

    half = lanes
    tri_line = lax.broadcasted_iota(jnp.int32, (half, half), 0)
    tri_column = lax.broadcasted_iota(jnp.int32, (half, half), 1)
    upper = tri_line <= tri_column
    blank = jnp.zeros((half, half), jnp.bfloat16)
    depth2 = field.shape[1] * field.shape[2]
    cells = field.shape[3]

    def block(first, f, part):
        return gathered[pl.ds(first, ring), f, part].reshape(half, half)

    matrix[pl.ds(0, half), pl.ds(3 * half, half)] = blank
    matrix[pl.ds(half, half), pl.ds(0, half)] = blank
    matrix[pl.ds(2 * half, half), pl.ds(half, half)] = blank
    matrix[pl.ds(3 * half, half), pl.ds(2 * half, half)] = blank

    def put(i, j, value):
        matrix[pl.ds(i * half, half), pl.ds(j * half, half)] = value

    def one_frequency(f, carry):
        for b in range(2):
            packed = block(b * ring, f, 0).astype(jnp.float32)
            sym = jnp.where(upper, packed, 0.0).astype(jnp.bfloat16)
            skew = jnp.where(upper, 0.0, packed)
            put(b, b, sym)
            put(2 + b, 2 + b, sym)
            put(2 + b, b, skew.astype(jnp.bfloat16))
            put(b, 2 + b, (-skew).astype(jnp.bfloat16))
        across = block(0, f, 1)
        put(0, 1, across)
        put(2, 3, across)
        below = block(ring, f, 1)
        put(3, 0, below)
        put(1, 2, -below)
        v = field[f].reshape(depth2, cells)
        image = jnp.dot(matrix[...], v, preferred_element_type=jnp.float32)
        power = jnp.sum((v.astype(jnp.float32) * image).reshape(depth2 // 8, 8, cells), axis=0)
        acc[...] += power * weight[pl.ds(f, 1), :]
        return carry

    def compute(c):
        for copy in two[c]:
            copy.wait_recv()
        loads[c].wait()
        lax.fori_loop(starts[c], starts[c] + CHUNKS[c][0], one_frequency, 0)

    for c in range(min(AHEAD, chunks)):
        issue_zero(c)
    for step in range(chunks + 2):
        if step < chunks:
            issue_one(step)
            if step + AHEAD < chunks:
                issue_zero(step + AHEAD)
        if 0 <= step - 1 < chunks:
            issue_two(step - 1)
        if 0 <= step - 2 < chunks:
            compute(step - 2)

    total = 2.0 / (n_freq * field.shape[0])
    sums[freq] = jnp.sum(acc[...], axis=0, keepdims=True) * total
    for c in range(chunks):
        for copy in (*zero[c], *one[c], *two[c]):
            copy.wait_send()
    copies = []
    for step in range(1, n_freq):
        copies.append(pltpu.make_async_remote_copy(
            src_ref=sums.at[freq], dst_ref=sums.at[freq],
            send_sem=sum_send.at[step], recv_sem=sum_recv.at[step],
            device_id={"freq": lax.rem(freq + step, n_freq)}, device_id_type=MESH,
        ))
        copies[-1].start()
    for copy in copies:
        copy.wait_recv()
    ambiguity = jnp.sum(sums[...], axis=0)
    peak = jnp.max(ambiguity, axis=1, keepdims=True)
    peaks[cell] = jnp.broadcast_to(peak, peaks.shape[1:])
    for copy in copies:
        copy.wait_send()
    copies = []
    for step in range(1, n_cell):
        copies.append(pltpu.make_async_remote_copy(
            src_ref=peaks.at[cell], dst_ref=peaks.at[cell],
            send_sem=peak_send.at[step], recv_sem=peak_recv.at[step],
            device_id={"cell": lax.rem(cell + step, n_cell)}, device_id_type=MESH,
        ))
        copies[-1].start()
    out_ref[0:1, :] = ambiguity
    for copy in copies:
        copy.wait_recv()
    top = jnp.max(jnp.max(peaks[...], axis=0), axis=1, keepdims=True)
    out_ref[1:2, :] = ambiguity / jnp.maximum(top, 1.0)
    for copy in copies:
        copy.wait_send()


def shards(covariance, replica, transmission):
    freqs, _, rows, depth = covariance.shape
    cells = replica.shape[3]
    n_freq, n_cell = lax.axis_size("freq"), lax.axis_size("cell")
    out = pl.pallas_call(
        kernel,
        out_shape=jax.ShapeDtypeStruct((2, cells), jnp.float32),
        in_specs=[pl.BlockSpec(memory_space=pltpu.HBM)] * 3,
        out_specs=pl.BlockSpec(memory_space=pltpu.VMEM),
        scratch_shapes=[
            pltpu.VMEM((freqs, 2, rows, depth // 2), jnp.bfloat16),
            pltpu.VMEM((n_cell, freqs, 2, rows, depth // 2), jnp.bfloat16),
            pltpu.VMEM((freqs, 2, depth, cells), jnp.bfloat16),
            pltpu.VMEM((freqs, cells), jnp.bfloat16),
            pltpu.VMEM((freqs, cells), jnp.float32),
            pltpu.VMEM((2 * depth, 2 * depth), jnp.bfloat16),
            pltpu.VMEM((8, cells), jnp.float32),
            pltpu.VMEM((n_freq, 1, cells), jnp.float32),
            pltpu.VMEM((n_cell, 1, 128), jnp.float32),
            pltpu.SemaphoreType.DMA((3,)),
            pltpu.SemaphoreType.DMA((len(CHUNKS),)),
            pltpu.SemaphoreType.DMA((len(CHUNKS), KINDS)),
            pltpu.SemaphoreType.DMA((len(CHUNKS), KINDS)),
            pltpu.SemaphoreType.DMA((n_freq,)),
            pltpu.SemaphoreType.DMA((n_freq,)),
            pltpu.SemaphoreType.DMA((n_cell,)),
            pltpu.SemaphoreType.DMA((n_cell,)),
        ],
        compiler_params=pltpu.CompilerParams(collective_id=0, has_side_effects=True),
    )(covariance, replica, transmission)
    return out[0], out[1]


def solution(mesh):
    return jax.shard_map(
        shards,
        mesh=mesh,
        in_specs=(P("freq", None, "cell", None), P("freq", None, None, "cell"), P("freq", "cell")),
        out_specs=(P("cell"), P("cell")),
        check_vma=False,
    )
```

```python
import functools

import jax
import jax.numpy as jnp
from jax import lax
from jax.experimental import pallas as pl
from jax.experimental.pallas import tpu as pltpu
from jax.sharding import PartitionSpec as P

MESH = pl.DeviceIdType.MESH
CHUNKS = 8
PATTERN = ((2, 2), (3, 1), (2, 2), (2, 2))
AHEAD = 3
SECOND = 2
THIRD = 5
KINDS = 12


def kernel(
    cov_hbm, rep_hbm, trans_hbm, out_ref,
    diag, gathered, field, trans, weight, matrix, acc, sums, peaks,
    load_sem, rep_sem, send_sem, recv_sem, sum_send, sum_recv, peak_send, peak_recv,
):
    freq, cell = lax.axis_index("freq"), lax.axis_index("cell")
    n_freq, n_cell = lax.axis_size("freq"), lax.axis_size("cell")
    ring = n_cell // 2
    x, row = lax.rem(cell, ring), lax.div(cell, ring)

    def at(shift, other=False):
        r = 1 - row if other else row
        return r * ring + lax.rem(x + shift + ring, ring)

    lanes = gathered.shape[-1]
    own = pl.ds(pl.multiple_of(row * lanes, lanes), lanes)
    far = pl.ds(pl.multiple_of((1 - row) * lanes, lanes), lanes)
    diag_load = pltpu.make_async_copy(cov_hbm.at[:, :, :, own], diag, load_sem.at[0])
    far_load = pltpu.make_async_copy(
        cov_hbm.at[:, row, :, far], gathered.at[cell, :, 1], load_sem.at[1]
    )
    trans_load = pltpu.make_async_copy(trans_hbm, trans, load_sem.at[2])
    diag_load.start()
    far_load.start()
    trans_load.start()
    period = len(PATTERN)
    offsets = [sum(sum(p) for p in PATTERN[:i]) for i in range(period + 1)]

    def load(c, k):
        part = pl.ds(lax.div(c, period) * offsets[-1] + offsets[k], sum(PATTERN[k]))
        return pltpu.make_async_copy(rep_hbm.at[part], field.at[part], rep_sem.at[c])

    def load_one(i, carry):
        for k in range(period):
            load(i * period + k, k).start()
        return carry

    lax.fori_loop(0, CHUNKS // period, load_one, 0)

    barrier = pltpu.get_barrier_semaphore()
    def greet(axis, me, n):
        def one(step, carry):
            pl.semaphore_signal(
                barrier, inc=1, device_id={axis: lax.rem(me + step, n)}, device_id_type=MESH
            )
            return carry

        lax.fori_loop(1, n, one, 0)

    greet("freq", freq, n_freq)
    greet("cell", cell, n_cell)

    diag_load.wait()
    shape = diag.shape[2:]
    line = lax.broadcasted_iota(jnp.int32, shape, 0) + x * shape[0]
    column = lax.broadcasted_iota(jnp.int32, shape, 1)
    factor = jnp.where(line == column, 0.5, 1.0).astype(jnp.float32)
    above = line <= column

    def pack(f, carry):
        re = diag[f, 0].astype(jnp.float32) * factor
        im = diag[f, 1].astype(jnp.float32)
        gathered[cell, f, 0] = jnp.where(above, re, im).astype(jnp.bfloat16)
        return carry

    lax.fori_loop(0, diag.shape[0], pack, 0, unroll=4)
    trans_load.wait()
    amplitude = trans[...].astype(jnp.float32)
    weight[...] = amplitude * amplitude
    acc[...] = jnp.zeros_like(acc)
    far_load.wait()
    pl.semaphore_wait(barrier, n_freq + n_cell - 2)

    right, left, partner = at(1), at(-1), at(0, True)
    TO_PARTNER, TO_RIGHT, TO_LEFT = 0, 1, 2
    ON_RIGHT, LEFT_OVER, ON_LEFT, RIGHT_OVER, OTHER_RIGHT, OTHER_LEFT = 3, 4, 5, 6, 7, 8
    FAR_OVER, OTHER_ON_RIGHT, OTHER_ON_LEFT = 9, 10, 11

    def kinds(k):
        by_x, by_y = PATTERN[k]
        size = by_x + by_y
        mid, mid_x = (size + k % 2) // 2, (by_x + 1 - k % 2) // 2
        table = {
            TO_PARTNER: (cell, partner, 0, size),
            TO_RIGHT: (cell, right, 0, size),
            TO_LEFT: (cell, left, 0, size),
            ON_RIGHT: (left, right, 0, mid),
            LEFT_OVER: (left, partner, by_x, by_y),
            ON_LEFT: (right, left, mid, size - mid),
            RIGHT_OVER: (right, partner, by_x, by_y),
            OTHER_RIGHT: (partner, right, 0, by_x),
            OTHER_LEFT: (partner, left, 0, by_x),
            FAR_OVER: (at(2), partner, by_x, by_y),
            OTHER_ON_RIGHT: (at(-1, True), right, 0, mid_x),
            OTHER_ON_LEFT: (at(1, True), left, mid_x, by_x - mid_x),
        }
        return {kind: row for kind, row in table.items() if row[3]}

    def copy_of(c, k, kind):
        piece, target, first, size = kinds(k)[kind]
        begin = lax.div(c, period) * offsets[-1] + offsets[k] + first
        ref = gathered.at[piece, pl.ds(begin, size)]
        return pltpu.make_async_remote_copy(
            src_ref=ref, dst_ref=ref,
            send_sem=send_sem.at[c, kind], recv_sem=recv_sem.at[c, kind],
            device_id={"cell": target}, device_id_type=MESH,
        )

    def start(c, k, *wanted):
        for kind in wanted:
            if kind in kinds(k):
                copy_of(c, k, kind).start()

    def arrived(c, k, *wanted):
        for kind in wanted:
            if kind in kinds(k):
                copy_of(c, k, kind).wait_recv()

    def issue_zero(c, k):
        start(c, k, TO_PARTNER, TO_RIGHT, TO_LEFT)

    def issue_one(c, k):
        arrived(c, k, TO_RIGHT)
        start(c, k, ON_RIGHT, LEFT_OVER)
        arrived(c, k, TO_LEFT)
        start(c, k, ON_LEFT, RIGHT_OVER)
        arrived(c, k, TO_PARTNER)
        start(c, k, OTHER_RIGHT, OTHER_LEFT)

    def issue_two(c, k):
        arrived(c, k, ON_RIGHT, ON_LEFT)
        start(c, k, FAR_OVER)
        arrived(c, k, OTHER_RIGHT)
        start(c, k, OTHER_ON_RIGHT)
        arrived(c, k, OTHER_LEFT)
        start(c, k, OTHER_ON_LEFT)
        arrived(c, k, LEFT_OVER, RIGHT_OVER)

    half = lanes
    tri_line = lax.broadcasted_iota(jnp.int32, (half, half), 0)
    tri_column = lax.broadcasted_iota(jnp.int32, (half, half), 1)
    upper = tri_line <= tri_column
    blank = jnp.zeros((half, half), jnp.bfloat16)
    depth2 = field.shape[1] * field.shape[2]
    cells = field.shape[3]

    def block(first, f, part):
        return gathered[pl.ds(first, ring), f, part].reshape(half, half)

    for slot in range(2):
        for i, j in ((0, 3), (1, 0), (2, 1), (3, 2)):
            matrix[slot, pl.ds(i * half, half), pl.ds(j * half, half)] = blank

    def one_frequency(f, slot):
        def put(i, j, value):
            matrix[slot, pl.ds(i * half, half), pl.ds(j * half, half)] = value

        for b in range(2):
            packed = block(b * ring, f, 0)
            sym = jnp.where(upper, packed, blank)
            skew = jnp.where(upper, blank, packed)
            put(b, b, sym)
            put(2 + b, 2 + b, sym)
            put(2 + b, b, skew)
            put(b, 2 + b, -skew)
        across = block(0, f, 1)
        put(0, 1, across)
        put(2, 3, across)
        below = block(ring, f, 1)
        put(3, 0, below)
        put(1, 2, -below)
        v = field[f].reshape(depth2, cells)
        image = jnp.dot(matrix[slot], v, preferred_element_type=jnp.float32)
        power = jnp.sum((v.astype(jnp.float32) * image).reshape(depth2 // 8, 8, cells), axis=0)
        return power * weight[pl.ds(f, 1), :]

    def compute(c, k, second):
        if not second:
            arrived(c, k, FAR_OVER, OTHER_ON_RIGHT, OTHER_ON_LEFT)
            load(c, k).wait()
        size = sum(PATTERN[k])
        half_size = size // 2
        f = lax.div(c, period) * offsets[-1] + offsets[k] + second * half_size
        if half_size == 1:
            acc[...] += one_frequency(f, 0)
        else:
            acc[...] += one_frequency(f, 0) + one_frequency(f + 1, 1)

    for c in range(AHEAD):
        issue_zero(c, c % period)

    def steps(i, carry):
        for k in range(period):
            step = i * period + k

            @pl.when(step + AHEAD < CHUNKS)
            def _():
                issue_zero(step + AHEAD, (k + AHEAD) % period)

            @pl.when(step < CHUNKS)
            def _():
                issue_one(step, k)

            @pl.when(jnp.logical_and(step >= THIRD, step - THIRD < CHUNKS))
            def _():
                compute(step - THIRD, (k - THIRD) % period, 0)

            @pl.when(jnp.logical_and(step >= SECOND, step - SECOND < CHUNKS))
            def _():
                issue_two(step - SECOND, (k - SECOND) % period)

            @pl.when(jnp.logical_and(step >= THIRD, step - THIRD < CHUNKS))
            def _():
                compute(step - THIRD, (k - THIRD) % period, 1)

        return carry

    lax.fori_loop(0, -(-(CHUNKS + THIRD) // period), steps, 0)

    def spread(ref, axis, me, n, ssem, rsem):
        def copy(step):
            return pltpu.make_async_remote_copy(
                src_ref=ref.at[me], dst_ref=ref.at[me],
                send_sem=ssem.at[step], recv_sem=rsem.at[step],
                device_id={axis: lax.rem(me + step, n)}, device_id_type=MESH,
            )

        def each(act):
            def one(step, carry):
                act(copy(step))
                return carry

            return lambda: lax.fori_loop(1, n, one, 0)

        return (
            each(lambda c: c.start()), each(lambda c: c.wait_recv()), each(lambda c: c.wait_send())
        )

    def sent(i, carry):
        for k in range(period):
            for kind in kinds(k):
                copy_of(i * period + k, k, kind).wait_send()
        return carry

    total = 2.0 / (n_freq * field.shape[0])
    sums[freq] = jnp.sum(acc[...], axis=0, keepdims=True) * total
    go, got, gone = spread(sums, "freq", freq, n_freq, sum_send, sum_recv)
    go()
    lax.fori_loop(0, CHUNKS // period, sent, 0)
    got()
    ambiguity = jnp.sum(sums[...], axis=0)
    peak = jnp.max(ambiguity, axis=1, keepdims=True)
    peaks[cell] = jnp.broadcast_to(peak, peaks.shape[1:])
    go_peak, got_peak, gone_peak = spread(peaks, "cell", cell, n_cell, peak_send, peak_recv)
    go_peak()
    gone()
    out_ref[0:1, :] = ambiguity
    got_peak()
    top = jnp.max(jnp.max(peaks[...], axis=0), axis=1, keepdims=True)
    out_ref[1:2, :] = ambiguity / jnp.maximum(top, 1.0)
    gone_peak()


def shards(covariance, replica, transmission):
    freqs, _, rows, depth = covariance.shape
    cells = replica.shape[3]
    n_freq, n_cell = lax.axis_size("freq"), lax.axis_size("cell")
    out = pl.pallas_call(
        kernel,
        out_shape=jax.ShapeDtypeStruct((2, cells), jnp.float32),
        in_specs=[pl.BlockSpec(memory_space=pltpu.HBM)] * 3,
        out_specs=pl.BlockSpec(memory_space=pltpu.VMEM),
        scratch_shapes=[
            pltpu.VMEM((freqs, 2, rows, depth // 2), jnp.bfloat16),
            pltpu.VMEM((n_cell, freqs, 2, rows, depth // 2), jnp.bfloat16),
            pltpu.VMEM((freqs, 2, depth, cells), jnp.bfloat16),
            pltpu.VMEM((freqs, cells), jnp.bfloat16),
            pltpu.VMEM((freqs, cells), jnp.float32),
            pltpu.VMEM((2, 2 * depth, 2 * depth), jnp.bfloat16),
            pltpu.VMEM((8, cells), jnp.float32),
            pltpu.VMEM((n_freq, 1, cells), jnp.float32),
            pltpu.VMEM((n_cell, 1, 128), jnp.float32),
            pltpu.SemaphoreType.DMA((3,)),
            pltpu.SemaphoreType.DMA((CHUNKS,)),
            pltpu.SemaphoreType.DMA((CHUNKS, KINDS)),
            pltpu.SemaphoreType.DMA((CHUNKS, KINDS)),
            pltpu.SemaphoreType.DMA((n_freq,)),
            pltpu.SemaphoreType.DMA((n_freq,)),
            pltpu.SemaphoreType.DMA((n_cell,)),
            pltpu.SemaphoreType.DMA((n_cell,)),
        ],
        compiler_params=pltpu.CompilerParams(collective_id=0, has_side_effects=True, vmem_limit_bytes=40 * 2**20),
    )(*[pltpu.with_memory_space_constraint(a, pltpu.HBM) for a in (covariance, replica, transmission)])
    return out[0], out[1]


def solution(mesh):
    return jax.shard_map(
        shards,
        mesh=mesh,
        in_specs=(P("freq", None, "cell", None), P("freq", None, None, "cell"), P("freq", "cell")),
        out_specs=(P("cell"), P("cell")),
        check_vma=False,
    )
```

```python
import functools

import jax
import jax.numpy as jnp
from jax import lax
from jax.experimental import pallas as pl
from jax.experimental.pallas import tpu as pltpu
from jax.sharding import PartitionSpec as P

MESH = pl.DeviceIdType.MESH
CHUNKS = 8
PIECES = 16
BY_X = 9
AHEAD = 3
SECOND = 2
THIRD = 5
KINDS = 12
CORES, Y_LOW = 2, 2


def kernel(
    cov_hbm, rep_hbm, trans_hbm, out_ref,
    diag, far, gathered, field, trans, weight, matrix, acc, sums, parts,
    load_sem, rep_sem, send_sem, recv_sem, sum_send, sum_recv, part_send, part_recv, word,
):
    freq, cell = lax.axis_index("freq"), lax.axis_index("cell")
    n_cell = lax.axis_size("cell")
    ring = n_cell // 2
    x, row = lax.rem(cell, ring), lax.div(cell, ring)

    def at(shift, other=False):
        r = 1 - row if other else row
        return r * ring + lax.rem(x + shift + ring, ring)

    lanes = gathered.shape[-1]
    freqs = field.shape[0]
    per_freq = gathered.shape[1] // freqs
    size = freqs // CHUNKS
    own = pl.ds(pl.multiple_of(row * lanes, lanes), lanes)
    other = pl.ds(pl.multiple_of((1 - row) * lanes, lanes), lanes)
    row_loads = []
    for i, part in enumerate((pl.ds(0, size), pl.ds(size, freqs - size))):
        row_loads.append((
            pltpu.make_async_copy(cov_hbm.at[part, :, :, own], diag.at[part], load_sem.at[2 * i]),
            pltpu.make_async_copy(
                cov_hbm.at[part, row, :, other], far.at[part], load_sem.at[2 * i + 1]
            ),
        ))
        for copy in row_loads[-1]:
            copy.start()
    trans_load = pltpu.make_async_copy(trans_hbm, trans, load_sem.at[4])
    trans_load.start()

    def load(c):
        part = pl.ds(c * size, size)
        return pltpu.make_async_copy(rep_hbm.at[part], field.at[part], rep_sem.at[c])

    def load_one(c, carry):
        load(c).start()
        return carry

    lax.fori_loop(0, CHUNKS, load_one, 0)

    core, y_low = lax.rem(freq, CORES), lax.rem(lax.div(freq, CORES), Y_LOW)
    z = lax.div(freq, CORES * Y_LOW)
    me_sum, n_sum = z * CORES + core, sums.shape[0]
    me_part, n_part = cell * Y_LOW + y_low, parts.shape[0]

    def sum_peer(step):
        j = lax.rem(me_sum + step, n_sum)
        return {"freq": (lax.div(j, CORES) * Y_LOW + y_low) * CORES + lax.rem(j, CORES)}

    def part_peer(step):
        j = lax.rem(me_part + step, n_part)
        return {
            "freq": (z * Y_LOW + lax.rem(j, Y_LOW)) * CORES + core, "cell": lax.div(j, Y_LOW)
        }

    barrier = pltpu.get_barrier_semaphore()

    n_z = n_sum // CORES
    freq_at = lambda zz, yy, cc: {"freq": (zz * Y_LOW + yy) * CORES + cc}
    neighbours = (
        {"cell": at(1)}, {"cell": at(-1)}, {"cell": at(0, True)},
        freq_at(z, y_low, 1 - core),
        freq_at(lax.rem(z + 1, n_z), y_low, core), freq_at(lax.rem(z + n_z - 1, n_z), y_low, core),
        freq_at(z, 1 - y_low, core),
        {**freq_at(z, 1 - y_low, core), "cell": at(0, True)},
    )

    def greet(semaphore):
        for target in neighbours:
            pl.semaphore_signal(semaphore, inc=1, device_id=target, device_id_type=MESH)

    greet(barrier)

    shape = diag.shape[2:]
    rows = shape[0] // 2
    line = lax.broadcasted_iota(jnp.int32, shape, 0) + x * shape[0]
    column = lax.broadcasted_iota(jnp.int32, shape, 1)
    factor = jnp.where(line == column, 0.5, 1.0).astype(jnp.bfloat16)
    above = line <= column

    def pack(f, carry):
        packed = jnp.where(above, diag[f, 0] * factor, diag[f, 1])
        across = far[f]
        for i in range(2):
            gathered[cell, per_freq * f + i] = packed[i * rows:(i + 1) * rows]
            gathered[cell, per_freq * f + 2 + i] = across[i * rows:(i + 1) * rows]
        return carry

    for copy in row_loads[0]:
        copy.wait()
    lax.fori_loop(0, size, pack, 0, unroll=4)

    right, left, partner = at(1), at(-1), at(0, True)
    TO_PARTNER, TO_RIGHT, TO_LEFT = 0, 1, 2
    ON_RIGHT, LEFT_OVER, ON_LEFT, RIGHT_OVER, OTHER_RIGHT, OTHER_LEFT = 3, 4, 5, 6, 7, 8
    FAR_OVER, OTHER_ON_RIGHT, OTHER_ON_LEFT = 9, 10, 11

    mid, mid_x, by_y = PIECES // 2, BY_X // 2, PIECES - BY_X
    table = {
        TO_PARTNER: (cell, partner, 0, PIECES),
        TO_RIGHT: (cell, right, 0, PIECES),
        TO_LEFT: (cell, left, 0, PIECES),
        ON_RIGHT: (left, right, 0, mid),
        LEFT_OVER: (left, partner, BY_X, by_y),
        ON_LEFT: (right, left, mid, PIECES - mid),
        RIGHT_OVER: (right, partner, BY_X, by_y),
        OTHER_RIGHT: (partner, right, 0, BY_X),
        OTHER_LEFT: (partner, left, 0, BY_X),
        FAR_OVER: (at(2), partner, BY_X, by_y),
        OTHER_ON_RIGHT: (at(-1, True), right, 0, mid_x),
        OTHER_ON_LEFT: (at(1, True), left, mid_x, BY_X - mid_x),
    }

    def copy_of(c, kind):
        source, target, first, count = table[kind]
        ref = gathered.at[source, pl.ds(c * PIECES + first, count)]
        return pltpu.make_async_remote_copy(
            src_ref=ref, dst_ref=ref,
            send_sem=send_sem.at[c, kind], recv_sem=recv_sem.at[c, kind],
            device_id={"cell": target}, device_id_type=MESH,
        )

    def start(c, *wanted):
        for kind in wanted:
            copy_of(c, kind).start()

    def arrived(c, *wanted):
        for kind in wanted:
            copy_of(c, kind).wait_recv()

    def issue_zero(c):
        start(c, TO_PARTNER, TO_RIGHT, TO_LEFT)

    def issue_one(c):
        arrived(c, TO_RIGHT)
        start(c, ON_RIGHT, LEFT_OVER)
        arrived(c, TO_LEFT)
        start(c, ON_LEFT, RIGHT_OVER)
        arrived(c, TO_PARTNER)
        start(c, OTHER_RIGHT, OTHER_LEFT)

    def issue_two(c):
        arrived(c, ON_RIGHT, ON_LEFT)
        start(c, FAR_OVER)
        arrived(c, OTHER_RIGHT)
        start(c, OTHER_ON_RIGHT)
        arrived(c, OTHER_LEFT)
        start(c, OTHER_ON_LEFT)
        arrived(c, LEFT_OVER, RIGHT_OVER)

    pl.semaphore_wait(barrier, len(neighbours))
    issue_zero(0)
    greet(word.at[0])
    for copy in row_loads[1]:
        copy.wait()
    lax.fori_loop(size, freqs, pack, 0, unroll=4)
    trans_load.wait()
    amplitude = trans[...].astype(jnp.float32)
    weight[...] = amplitude * amplitude
    acc[...] = jnp.zeros_like(acc)

    half = lanes
    tri_line = lax.broadcasted_iota(jnp.int32, (half, half), 0)
    tri_column = lax.broadcasted_iota(jnp.int32, (half, half), 1)
    upper = tri_line <= tri_column
    blank = jnp.zeros((half, half), jnp.bfloat16)
    depth2 = field.shape[1] * field.shape[2]
    cells = field.shape[3]

    def block(first, f, part):
        return gathered[pl.ds(first, ring), pl.ds(per_freq * f + 2 * part, 2)].reshape(half, half)

    for slot in range(2):
        for i, j in ((0, 3), (1, 0), (2, 1), (3, 2)):
            matrix[slot, pl.ds(i * half, half), pl.ds(j * half, half)] = blank

    def one_frequency(f, slot):
        def put(i, j, value):
            matrix[slot, pl.ds(i * half, half), pl.ds(j * half, half)] = value

        for b in range(2):
            packed = block(b * ring, f, 0)
            sym = jnp.where(upper, packed, blank)
            skew = jnp.where(upper, blank, packed)
            put(b, b, sym)
            put(2 + b, 2 + b, sym)
            put(2 + b, b, skew)
            put(b, 2 + b, -skew)
        across = block(0, f, 1)
        put(0, 1, across)
        put(2, 3, across)
        below = block(ring, f, 1)
        put(3, 0, below)
        put(1, 2, -below)
        v = field[f].reshape(depth2, cells)
        image = jnp.dot(matrix[slot], v, preferred_element_type=jnp.float32)
        power = jnp.sum((v.astype(jnp.float32) * image).reshape(depth2 // 8, 8, cells), axis=0)
        return power * weight[pl.ds(f, 1), :]

    def compute(c, second):
        if not second:
            arrived(c, FAR_OVER, OTHER_ON_RIGHT, OTHER_ON_LEFT)
            load(c).wait()
        f = c * size + second * 2
        acc[...] += one_frequency(f, 0) + one_frequency(f + 1, 1)

    for c in range(1, AHEAD):
        issue_zero(c)
    pl.semaphore_wait(word.at[0], len(neighbours))
    greet(word.at[1])

    def steps(step, carry):
        ready = jnp.logical_and(step >= THIRD, step - THIRD < CHUNKS)

        @pl.when(ready)
        def _():
            compute(step - THIRD, 0)

        @pl.when(step + AHEAD < CHUNKS)
        def _():
            issue_zero(step + AHEAD)

        @pl.when(step < CHUNKS)
        def _():
            issue_one(step)

        @pl.when(jnp.logical_and(step >= SECOND, step - SECOND < CHUNKS))
        def _():
            issue_two(step - SECOND)

        @pl.when(ready)
        def _():
            compute(step - THIRD, 1)

        return carry

    lax.fori_loop(0, CHUNKS + THIRD, steps, 0)

    pl.semaphore_wait(word.at[1], len(neighbours))

    def spread(ref, me, peer, ssem, rsem):
        n = ref.shape[0]

        def copy(step):
            return pltpu.make_async_remote_copy(
                src_ref=ref.at[me], dst_ref=ref.at[me],
                send_sem=ssem.at[step], recv_sem=rsem.at[step],
                device_id=peer(step), device_id_type=MESH,
            )

        def each(act):
            def one(step, carry):
                act(copy(step))
                return carry

            return lambda: lax.fori_loop(1, n, one, 0)

        return (
            each(lambda c: c.start()), each(lambda c: c.wait_recv()), each(lambda c: c.wait_send())
        )

    def sent(c, carry):
        for kind in table:
            copy_of(c, kind).wait_send()
        return carry

    total = 2.0 / (lax.axis_size("freq") * freqs)
    sums[me_sum] = jnp.sum(acc[...], axis=0, keepdims=True) * total
    go, got, gone = spread(sums, me_sum, sum_peer, sum_send, sum_recv)
    go()
    lax.fori_loop(0, CHUNKS, sent, 0)
    got()
    parts[me_part] = jnp.sum(sums[...], axis=0)
    go_part, got_part, gone_part = spread(parts, me_part, part_peer, part_send, part_recv)
    go_part()
    gone()
    got_part()
    ambiguity = parts[cell * Y_LOW] + parts[cell * Y_LOW + 1]
    everywhere = jnp.sum(parts[...].reshape(n_cell, Y_LOW, cells), axis=1)
    peak = jnp.max(jnp.max(everywhere, axis=0, keepdims=True), axis=1, keepdims=True)
    out_ref[0:1, :] = ambiguity
    out_ref[1:2, :] = ambiguity / jnp.maximum(peak, 1.0)
    gone_part()


def shards(covariance, replica, transmission):
    freqs, _, rows, depth = covariance.shape
    cells = replica.shape[3]
    n_freq, n_cell = lax.axis_size("freq"), lax.axis_size("cell")
    out = pl.pallas_call(
        kernel,
        out_shape=jax.ShapeDtypeStruct((2, cells), jnp.float32),
        in_specs=[pl.BlockSpec(memory_space=pltpu.HBM)] * 3,
        out_specs=pl.BlockSpec(memory_space=pltpu.VMEM),
        scratch_shapes=[
            pltpu.VMEM((freqs, 2, rows, depth // 2), jnp.bfloat16),
            pltpu.VMEM((freqs, rows, depth // 2), jnp.bfloat16),
            pltpu.VMEM((n_cell, freqs * 4, rows // 2, depth // 2), jnp.bfloat16),
            pltpu.VMEM((freqs, 2, depth, cells), jnp.bfloat16),
            pltpu.VMEM((freqs, cells), jnp.bfloat16),
            pltpu.VMEM((freqs, cells), jnp.float32),
            pltpu.VMEM((2, 2 * depth, 2 * depth), jnp.bfloat16),
            pltpu.VMEM((8, cells), jnp.float32),
            pltpu.VMEM((n_freq // Y_LOW, 1, cells), jnp.float32),
            pltpu.VMEM((n_cell * Y_LOW, 1, cells), jnp.float32),
            pltpu.SemaphoreType.DMA((5,)),
            pltpu.SemaphoreType.DMA((CHUNKS,)),
            pltpu.SemaphoreType.DMA((CHUNKS, KINDS)),
            pltpu.SemaphoreType.DMA((CHUNKS, KINDS)),
            pltpu.SemaphoreType.DMA((n_freq // Y_LOW,)),
            pltpu.SemaphoreType.DMA((n_freq // Y_LOW,)),
            pltpu.SemaphoreType.DMA((n_cell * Y_LOW,)),
            pltpu.SemaphoreType.DMA((n_cell * Y_LOW,)),
            pltpu.SemaphoreType.REGULAR((2,)),
        ],
        compiler_params=pltpu.CompilerParams(collective_id=0, has_side_effects=True, vmem_limit_bytes=40 * 2**20),
    )(*[pltpu.with_memory_space_constraint(a, pltpu.HBM) for a in (covariance, replica, transmission)])
    return out[0], out[1]


def solution(mesh):
    return jax.shard_map(
        shards,
        mesh=mesh,
        in_specs=(P("freq", None, "cell", None), P("freq", None, None, "cell"), P("freq", "cell")),
        out_specs=(P("cell"), P("cell")),
        check_vma=False,
    )
```

```python
import functools

import jax
import jax.numpy as jnp
from jax import lax
from jax.experimental import pallas as pl
from jax.experimental.pallas import tpu as pltpu
from jax.sharding import PartitionSpec as P

MESH = pl.DeviceIdType.MESH
CHUNKS = 8
PIECES = 16
BY_X = 8
AHEAD = 4
PROGRAM = (
    ("over", 0),
    ("other", 2),
    ("x", 4),
    ("cx", 4),
    ("y", 5),
    ("far", 2),
    ("near", 0),
    ("send", -AHEAD),
    ("cy", 5),
)
PAIRS = {"cx": (0, 1), "cy": (2, 3)}
FIRST = "cx"
GROUPS = 6
CORES, Y_LOW = 2, 2


def kernel(
    cov_hbm, rep_hbm, trans_hbm, out_ref,
    diag, far, gathered, field, trans, weight, matrix, acc, sums, parts,
    load_sem, rep_sem, send_sem, recv_sem, sum_sem, part_sem, word,
):
    freq, cell = lax.axis_index("freq"), lax.axis_index("cell")
    n_cell = lax.axis_size("cell")
    ring = n_cell // 2
    x, row = lax.rem(cell, ring), lax.div(cell, ring)

    def at(shift, other=False):
        r = 1 - row if other else row
        return r * ring + lax.rem(x + shift + ring, ring)

    core, y_low = lax.rem(freq, CORES), lax.rem(lax.div(freq, CORES), Y_LOW)
    z = lax.div(freq, CORES * Y_LOW)
    me_sum, n_sum = z * CORES + core, sums.shape[0]
    me_part, n_part = cell * Y_LOW + y_low, parts.shape[0]

    def sum_peer(step):
        j = lax.rem(me_sum + step, n_sum)
        return {"freq": (lax.div(j, CORES) * Y_LOW + y_low) * CORES + lax.rem(j, CORES)}

    def part_peer(step):
        j = lax.rem(me_part + step, n_part)
        return {
            "freq": (z * Y_LOW + lax.rem(j, Y_LOW)) * CORES + core, "cell": lax.div(j, Y_LOW)
        }

    barrier = pltpu.get_barrier_semaphore()

    n_z = n_sum // CORES
    freq_at = lambda zz, yy, cc: {"freq": (zz * Y_LOW + yy) * CORES + cc}
    neighbours = (
        {"cell": at(1)}, {"cell": at(-1)}, {"cell": at(0, True)},
        freq_at(z, y_low, 1 - core),
        freq_at(lax.rem(z + 1, n_z), y_low, core), freq_at(lax.rem(z + n_z - 1, n_z), y_low, core),
        freq_at(z, 1 - y_low, core),
        {**freq_at(z, 1 - y_low, core), "cell": at(0, True)},
    )

    def greet(semaphore):
        for target in neighbours:
            pl.semaphore_signal(semaphore, inc=1, device_id=target, device_id_type=MESH)

    greet(barrier)

    lanes = gathered.shape[-1]
    freqs = field.shape[0]
    per_freq = gathered.shape[1] // freqs
    size = freqs // CHUNKS
    own = pl.ds(pl.multiple_of(row * lanes, lanes), lanes)
    other = pl.ds(pl.multiple_of((1 - row) * lanes, lanes), lanes)
    row_loads = []
    for i, part in enumerate((pl.ds(0, size), pl.ds(size, freqs - size))):
        row_loads.append((
            pltpu.make_async_copy(cov_hbm.at[part, :, :, own], diag.at[part], load_sem.at[2 * i]),
            pltpu.make_async_copy(
                cov_hbm.at[part, row, :, other], far.at[part], load_sem.at[2 * i + 1]
            ),
        ))
        for copy in row_loads[-1]:
            copy.start()
    trans_load = pltpu.make_async_copy(trans_hbm, trans, load_sem.at[4])
    trans_load.start()

    def load(c):
        part = pl.ds(c * size, size)
        return pltpu.make_async_copy(rep_hbm.at[part], field.at[part], rep_sem)

    def load_one(c, carry):
        load(c).start()
        return carry

    lax.fori_loop(0, CHUNKS, load_one, 0)

    shape = diag.shape[2:]
    rows = shape[0] // 2
    line = lax.broadcasted_iota(jnp.int32, shape, 0) + x * shape[0]
    column = lax.broadcasted_iota(jnp.int32, shape, 1)
    factor = jnp.where(line == column, 0.5, 1.0).astype(jnp.bfloat16)
    above = line <= column

    def pack(f, carry):
        packed = jnp.where(above, diag[f, 0] * factor, diag[f, 1])
        across = far[f]
        for i in range(2):
            gathered[cell, per_freq * f + i] = packed[i * rows:(i + 1) * rows]
            gathered[cell, per_freq * f + 2 + i] = across[i * rows:(i + 1) * rows]
        return carry

    for copy in row_loads[0]:
        copy.wait()
    lax.fori_loop(0, size, pack, 0, unroll=4)

    right, left, partner = at(1), at(-1), at(0, True)
    TO_PARTNER, TO_RIGHT, TO_LEFT = 0, 1, 2
    ON_RIGHT, LEFT_OVER, ON_LEFT, RIGHT_OVER, OTHER_RIGHT, OTHER_LEFT = 3, 4, 5, 6, 7, 8
    FAR_OVER, OTHER_ON_RIGHT, OTHER_ON_LEFT = 9, 10, 11

    mid, mid_x, by_y = PIECES // 2, BY_X // 2, PIECES - BY_X
    table = {
        TO_PARTNER: (cell, partner, 0, PIECES),
        TO_RIGHT: (cell, right, 0, PIECES),
        TO_LEFT: (cell, left, 0, PIECES),
        ON_RIGHT: (left, right, 0, mid),
        LEFT_OVER: (left, partner, BY_X, by_y),
        ON_LEFT: (right, left, mid, PIECES - mid),
        RIGHT_OVER: (right, partner, BY_X, by_y),
        OTHER_RIGHT: (partner, right, 0, BY_X),
        OTHER_LEFT: (partner, left, 0, BY_X),
        FAR_OVER: (at(2), partner, BY_X, by_y),
        OTHER_ON_RIGHT: (at(-1, True), right, 0, mid_x),
        OTHER_ON_LEFT: (at(1, True), left, mid_x, BY_X - mid_x),
    }

    NEAR, OVER, ON, OTHER, BY_Y, LAST = range(6)
    group = {
        TO_RIGHT: NEAR, TO_LEFT: NEAR, TO_PARTNER: OVER, ON_RIGHT: ON, ON_LEFT: ON,
        OTHER_RIGHT: OTHER, OTHER_LEFT: OTHER, LEFT_OVER: BY_Y, RIGHT_OVER: BY_Y,
        FAR_OVER: BY_Y, OTHER_ON_RIGHT: LAST, OTHER_ON_LEFT: LAST,
    }
    landing = {
        NEAR: (pl.ds(0, 2), 0, PIECES),
        OVER: (partner, 0, PIECES),
        ON: (at(2), 0, PIECES),
        OTHER: (pl.ds(0, 2), 0, BY_X),
        BY_Y: (pl.ds(0, 3), BY_X, by_y),
        LAST: (at(2, True), 0, BY_X),
    }

    def start(c, *wanted):
        for kind in wanted:
            source, target, first, count = table[kind]
            ref = gathered.at[source, pl.ds(c * PIECES + first, count)]
            pltpu.make_async_remote_copy(
                src_ref=ref, dst_ref=ref,
                send_sem=send_sem, recv_sem=recv_sem.at[c, group[kind]],
                device_id={"cell": target}, device_id_type=MESH,
            ).start()

    def arrived(c, which):
        source, first, count = landing[which]
        ref = gathered.at[source, pl.ds(c * PIECES + first, count)]
        pltpu.make_async_copy(ref, ref, recv_sem.at[c, which]).wait()

    def issue_zero(c):
        start(c, TO_PARTNER, TO_RIGHT, TO_LEFT)

    actions = {
        "near": (NEAR, (ON_RIGHT, ON_LEFT, LEFT_OVER, RIGHT_OVER)),
        "over": (OVER, (OTHER_RIGHT, OTHER_LEFT)),
        "far": (ON, (FAR_OVER,)),
        "other": (OTHER, (OTHER_ON_RIGHT, OTHER_ON_LEFT)),
        "y": (BY_Y, ()),
        "x": (LAST, ()),
    }

    pl.semaphore_wait(barrier, len(neighbours))
    issue_zero(0)
    greet(word.at[0])
    for copy in row_loads[1]:
        copy.wait()
    lax.fori_loop(size, freqs, pack, 0, unroll=4)
    trans_load.wait()
    amplitude = trans[...].astype(jnp.float32)
    weight[...] = amplitude * amplitude
    acc[...] = jnp.zeros_like(acc)

    half = lanes
    tri_line = lax.broadcasted_iota(jnp.int32, (half, half), 0)
    tri_column = lax.broadcasted_iota(jnp.int32, (half, half), 1)
    upper = tri_line <= tri_column
    blank = jnp.zeros((half, half), jnp.bfloat16)
    depth2 = field.shape[1] * field.shape[2]
    cells = field.shape[3]

    def block(first, f, part):
        return gathered[pl.ds(first, ring), pl.ds(per_freq * f + 2 * part, 2)].reshape(half, half)

    for slot in range(2):
        for i, j in ((0, 3), (1, 0), (2, 1), (3, 2)):
            matrix[slot, pl.ds(i * half, half), pl.ds(j * half, half)] = blank

    def one_frequency(f, slot):
        def put(i, j, value):
            matrix[slot, pl.ds(i * half, half), pl.ds(j * half, half)] = value

        for b in range(2):
            packed = block(b * ring, f, 0)
            sym = jnp.where(upper, packed, blank)
            skew = jnp.where(upper, blank, packed)
            put(b, b, sym)
            put(2 + b, 2 + b, sym)
            put(2 + b, b, skew)
            put(b, 2 + b, -skew)
        across = block(0, f, 1)
        put(0, 1, across)
        put(2, 3, across)
        below = block(ring, f, 1)
        put(3, 0, below)
        put(1, 2, -below)
        v = field[f].reshape(depth2, cells)
        image = jnp.dot(matrix[slot], v, preferred_element_type=jnp.float32)
        power = jnp.sum((v.astype(jnp.float32) * image).reshape(depth2 // 8, 8, cells), axis=0)
        return power * weight[pl.ds(f, 1), :]

    def act(name, c):
        if name in PAIRS:
            if name == FIRST:

                @pl.when(c == 0)
                def _():
                    pltpu.make_async_copy(rep_hbm, field, rep_sem).wait()

            f, g = (c * size + offset for offset in PAIRS[name])
            acc[...] += one_frequency(f, 0) + one_frequency(g, 1)
            return
        which, starts = actions[name]
        arrived(c, which)
        start(c, *starts)

    for c in range(1, AHEAD):
        issue_zero(c)
    pl.semaphore_wait(word.at[0], len(neighbours))
    greet(word.at[1])

    def steps(step, carry):
        for name, lag in PROGRAM:
            c = step - lag
            if name == "send":
                pl.when(c < CHUNKS)(functools.partial(issue_zero, c))
            else:
                inside = jnp.logical_and(c >= 0, c < CHUNKS)
                pl.when(inside)(functools.partial(act, name, c))
        return carry

    lax.fori_loop(0, CHUNKS + max(lag for _, lag in PROGRAM), steps, 0)

    pl.semaphore_wait(word.at[1], len(neighbours))

    def spread(ref, me, peer, ssem, rsem):
        n = ref.shape[0]

        def one(step, carry):
            pltpu.make_async_remote_copy(
                src_ref=ref.at[me], dst_ref=ref.at[me], send_sem=ssem, recv_sem=rsem,
                device_id=peer(step), device_id_type=MESH,
            ).start()
            return carry

        lax.fori_loop(1, n, one, 0)

    def all_but_one(ref, semaphore):
        part = ref.at[pl.ds(0, ref.shape[0] - 1)]
        pltpu.make_async_copy(part, part, semaphore).wait()

    total = 2.0 / (lax.axis_size("freq") * freqs)
    sums[me_sum] = jnp.sum(acc[...], axis=0, keepdims=True) * total
    spread(sums, me_sum, sum_peer, sum_sem.at[0], sum_sem.at[1])
    all_but_one(gathered, send_sem)
    all_but_one(sums, sum_sem.at[1])
    parts[me_part] = jnp.sum(sums[...], axis=0)
    spread(parts, me_part, part_peer, part_sem.at[0], part_sem.at[1])
    all_but_one(sums, sum_sem.at[0])
    all_but_one(parts, part_sem.at[1])
    ambiguity = parts[cell * Y_LOW] + parts[cell * Y_LOW + 1]
    everywhere = jnp.sum(parts[...].reshape(n_cell, Y_LOW, cells), axis=1)
    peak = jnp.max(jnp.max(everywhere, axis=0, keepdims=True), axis=1, keepdims=True)
    out_ref[0:1, :] = ambiguity
    out_ref[1:2, :] = ambiguity / jnp.maximum(peak, 1.0)
    all_but_one(parts, part_sem.at[0])


def shards(covariance, replica, transmission):
    freqs, _, rows, depth = covariance.shape
    cells = replica.shape[3]
    n_freq, n_cell = lax.axis_size("freq"), lax.axis_size("cell")
    out = pl.pallas_call(
        kernel,
        out_shape=jax.ShapeDtypeStruct((2, cells), jnp.float32),
        in_specs=[pl.BlockSpec(memory_space=pltpu.HBM)] * 3,
        out_specs=pl.BlockSpec(memory_space=pltpu.VMEM),
        scratch_shapes=[
            pltpu.VMEM((freqs, 2, rows, depth // 2), jnp.bfloat16),
            pltpu.VMEM((freqs, rows, depth // 2), jnp.bfloat16),
            pltpu.VMEM((n_cell, freqs * 4, rows // 2, depth // 2), jnp.bfloat16),
            pltpu.VMEM((freqs, 2, depth, cells), jnp.bfloat16),
            pltpu.VMEM((freqs, cells), jnp.bfloat16),
            pltpu.VMEM((freqs, cells), jnp.float32),
            pltpu.VMEM((2, 2 * depth, 2 * depth), jnp.bfloat16),
            pltpu.VMEM((8, cells), jnp.float32),
            pltpu.VMEM((n_freq // Y_LOW, 1, cells), jnp.float32),
            pltpu.VMEM((n_cell * Y_LOW, 1, cells), jnp.float32),
            pltpu.SemaphoreType.DMA((5,)),
            pltpu.SemaphoreType.DMA,
            pltpu.SemaphoreType.DMA,
            pltpu.SemaphoreType.DMA((CHUNKS, GROUPS)),
            pltpu.SemaphoreType.DMA((2,)),
            pltpu.SemaphoreType.DMA((2,)),
            pltpu.SemaphoreType.REGULAR((2,)),
        ],
        compiler_params=pltpu.CompilerParams(collective_id=0, has_side_effects=True, vmem_limit_bytes=40 * 2**20),
    )(*[pltpu.with_memory_space_constraint(a, pltpu.HBM) for a in (covariance, replica, transmission)])
    return out[0], out[1]


def solution(mesh):
    return jax.shard_map(
        shards,
        mesh=mesh,
        in_specs=(P("freq", None, "cell", None), P("freq", None, None, "cell"), P("freq", "cell")),
        out_specs=(P("cell"), P("cell")),
        check_vma=False,
    )
```

```python
import functools

import jax
import jax.numpy as jnp
from jax import lax
from jax.experimental import pallas as pl
from jax.experimental.pallas import tpu as pltpu
from jax.sharding import PartitionSpec as P

MESH = pl.DeviceIdType.MESH
CHUNKS = 8
PIECES = 16
BY_X = 8
AHEAD = 4
PROGRAM = (
    ("over", 0),
    ("other", 2),
    ("x", 4),
    ("cx", 4),
    ("y", 5),
    ("far", 2),
    ("near", 0),
    ("send", -AHEAD),
    ("cy", 5),
)
PAIRS = {"cx": (0, 1), "cy": (2, 3)}
FIRST = "cx"
GROUPS = 6
CORES, Y_LOW = 2, 2


def kernel(
    cov_hbm, rep_hbm, trans_hbm, out_ref,
    diag, far, gathered, field, trans, weight, matrix, acc, sums, parts,
    load_sem, rep_sem, send_sem, recv_sem, sum_sem, part_sem, word,
):
    freq, cell = lax.axis_index("freq"), lax.axis_index("cell")
    n_cell = lax.axis_size("cell")
    ring = n_cell // 2
    x, row = lax.rem(cell, ring), lax.div(cell, ring)

    def at(shift, other=False):
        r = 1 - row if other else row
        return r * ring + lax.rem(x + shift + ring, ring)

    core, y_low = lax.rem(freq, CORES), lax.rem(lax.div(freq, CORES), Y_LOW)
    z = lax.div(freq, CORES * Y_LOW)
    me_sum, n_sum = z * CORES + core, sums.shape[0]
    me_part, n_part = cell * Y_LOW + y_low, parts.shape[0]

    def sum_peer(step):
        j = lax.rem(me_sum + step, n_sum)
        return {"freq": (lax.div(j, CORES) * Y_LOW + y_low) * CORES + lax.rem(j, CORES)}

    def part_peer(step):
        j = lax.rem(me_part + step, n_part)
        return {
            "freq": (z * Y_LOW + lax.rem(j, Y_LOW)) * CORES + core, "cell": lax.div(j, Y_LOW)
        }

    barrier = pltpu.get_barrier_semaphore()

    n_z = n_sum // CORES
    freq_at = lambda zz, yy, cc: {"freq": (zz * Y_LOW + yy) * CORES + cc}
    neighbours = (
        {"cell": at(1)}, {"cell": at(-1)}, {"cell": at(0, True)},
        freq_at(z, y_low, 1 - core),
        freq_at(lax.rem(z + 1, n_z), y_low, core), freq_at(lax.rem(z + n_z - 1, n_z), y_low, core),
        freq_at(z, 1 - y_low, core),
        {**freq_at(z, 1 - y_low, core), "cell": at(0, True)},
    )

    def greet(semaphore):
        for target in neighbours:
            pl.semaphore_signal(semaphore, inc=1, device_id=target, device_id_type=MESH)

    greet(barrier)

    def slot(shift, other=False):
        r, to = 1 - row if other else row, lax.rem(x + shift + ring, ring)
        return r * ring + lax.rem(to, 2) * (ring // 2) + lax.div(to, 2)

    beside = row * ring + (1 - lax.rem(x, 2)) * (ring // 2)

    lanes = gathered.shape[-1]
    freqs = field.shape[0]
    per_freq = gathered.shape[1] // freqs
    size = freqs // CHUNKS
    own = pl.ds(pl.multiple_of(row * lanes, lanes), lanes)
    other = pl.ds(pl.multiple_of((1 - row) * lanes, lanes), lanes)
    row_loads = []
    for i, part in enumerate((pl.ds(0, size), pl.ds(size, freqs - size))):
        row_loads.append((
            pltpu.make_async_copy(cov_hbm.at[part, :, :, own], diag.at[part], load_sem.at[2 * i]),
            pltpu.make_async_copy(
                cov_hbm.at[part, row, :, other], far.at[part], load_sem.at[2 * i + 1]
            ),
        ))
        for copy in row_loads[-1]:
            copy.start()
    trans_load = pltpu.make_async_copy(trans_hbm, trans, load_sem.at[4])
    trans_load.start()

    def load(c):
        part = pl.ds(c * size, size)
        return pltpu.make_async_copy(rep_hbm.at[part], field.at[part], rep_sem)

    def load_one(c, carry):
        load(c).start()
        return carry

    lax.fori_loop(0, CHUNKS, load_one, 0)

    shape = diag.shape[2:]
    rows = shape[0] // 2
    line = lax.broadcasted_iota(jnp.int32, shape, 0) + x * shape[0]
    column = lax.broadcasted_iota(jnp.int32, shape, 1)
    factor = jnp.where(line == column, 0.5, 1.0).astype(jnp.bfloat16)
    above = line <= column

    def pack(f, carry):
        packed = jnp.where(above, diag[f, 0] * factor, diag[f, 1])
        across = far[f]
        for i in range(2):
            gathered[slot(0), per_freq * f + i] = packed[i * rows:(i + 1) * rows]
            gathered[slot(0), per_freq * f + 2 + i] = across[i * rows:(i + 1) * rows]
        return carry

    for copy in row_loads[0]:
        copy.wait()
    lax.fori_loop(0, size, pack, 0, unroll=4)

    right, left, partner = at(1), at(-1), at(0, True)
    TO_PARTNER, TO_RIGHT, TO_LEFT, ON_RIGHT, ON_LEFT, BOTH_OVER = range(6)
    OTHER_RIGHT, OTHER_LEFT, FAR_OVER, OTHER_ON_RIGHT, OTHER_ON_LEFT = range(6, 11)
    NEAR, OVER, ON, OTHER, BY_Y, LAST = range(GROUPS)
    mid, mid_x, by_y = PIECES // 2, BY_X // 2, PIECES - BY_X
    table = {
        TO_PARTNER: (slot(0), partner, 0, PIECES, OVER),
        TO_RIGHT: (slot(0), right, 0, PIECES, NEAR),
        TO_LEFT: (slot(0), left, 0, PIECES, NEAR),
        ON_RIGHT: (slot(-1), right, 0, mid, ON),
        ON_LEFT: (slot(1), left, mid, PIECES - mid, ON),
        BOTH_OVER: (pl.ds(beside, 2), partner, BY_X, by_y, BY_Y),
        OTHER_RIGHT: (slot(0, True), right, 0, BY_X, OTHER),
        OTHER_LEFT: (slot(0, True), left, 0, BY_X, OTHER),
        FAR_OVER: (slot(2), partner, BY_X, by_y, BY_Y),
        OTHER_ON_RIGHT: (slot(-1, True), right, 0, mid_x, LAST),
        OTHER_ON_LEFT: (slot(1, True), left, mid_x, BY_X - mid_x, LAST),
    }
    landing = {
        NEAR: (pl.ds(0, 2), 0, PIECES),
        OVER: (slot(0, True), 0, PIECES),
        ON: (slot(2), 0, PIECES),
        OTHER: (pl.ds(0, 2), 0, BY_X),
        BY_Y: (pl.ds(0, 3), BY_X, by_y),
        LAST: (slot(2, True), 0, BY_X),
    }

    def start(c, *wanted):
        for kind in wanted:
            source, target, first, count, group = table[kind]
            ref = gathered.at[source, pl.ds(c * PIECES + first, count)]
            pltpu.make_async_remote_copy(
                src_ref=ref, dst_ref=ref,
                send_sem=send_sem, recv_sem=recv_sem.at[c, group],
                device_id={"cell": target}, device_id_type=MESH,
            ).start()

    def arrived(c, which):
        source, first, count = landing[which]
        ref = gathered.at[source, pl.ds(c * PIECES + first, count)]
        pltpu.make_async_copy(ref, ref, recv_sem.at[c, which]).wait()

    def issue_zero(c):
        start(c, TO_PARTNER, TO_RIGHT, TO_LEFT)

    actions = {
        "near": (NEAR, (ON_RIGHT, ON_LEFT, BOTH_OVER)),
        "over": (OVER, (OTHER_RIGHT, OTHER_LEFT)),
        "far": (ON, (FAR_OVER,)),
        "other": (OTHER, (OTHER_ON_RIGHT, OTHER_ON_LEFT)),
        "y": (BY_Y, ()),
        "x": (LAST, ()),
    }

    pl.semaphore_wait(barrier, len(neighbours))
    issue_zero(0)
    greet(word.at[0])
    for copy in row_loads[1]:
        copy.wait()
    lax.fori_loop(size, freqs, pack, 0, unroll=4)
    trans_load.wait()
    amplitude = trans[...].astype(jnp.float32)
    weight[...] = amplitude * amplitude
    acc[...] = jnp.zeros_like(acc)

    half = lanes
    tri_line = lax.broadcasted_iota(jnp.int32, (half, half), 0)
    tri_column = lax.broadcasted_iota(jnp.int32, (half, half), 1)
    upper = tri_line <= tri_column
    blank = jnp.zeros((half, half), jnp.bfloat16)
    depth2 = field.shape[1] * field.shape[2]
    cells = field.shape[3]

    def block(first, f, part):
        pieces = pl.ds(per_freq * f + 2 * part, 2)
        order = [first + to % 2 * (ring // 2) + to // 2 for to in range(ring)]
        return jnp.concatenate(
            [gathered[i, pieces].reshape(half // ring, half) for i in order]
        )

    for slot in range(2):
        for i, j in ((0, 3), (1, 0), (2, 1), (3, 2)):
            matrix[slot, pl.ds(i * half, half), pl.ds(j * half, half)] = blank

    def one_frequency(f, slot):
        def put(i, j, value):
            matrix[slot, pl.ds(i * half, half), pl.ds(j * half, half)] = value

        for b in range(2):
            packed = block(b * ring, f, 0)
            sym = jnp.where(upper, packed, blank)
            skew = jnp.where(upper, blank, packed)
            put(b, b, sym)
            put(2 + b, 2 + b, sym)
            put(2 + b, b, skew)
            put(b, 2 + b, -skew)
        across = block(0, f, 1)
        put(0, 1, across)
        put(2, 3, across)
        below = block(ring, f, 1)
        put(3, 0, below)
        put(1, 2, -below)
        v = field[f].reshape(depth2, cells)
        image = jnp.dot(matrix[slot], v, preferred_element_type=jnp.float32)
        power = jnp.sum((v.astype(jnp.float32) * image).reshape(depth2 // 8, 8, cells), axis=0)
        return power * weight[pl.ds(f, 1), :]

    def act(name, c):
        if name in PAIRS:
            if name == FIRST:

                @pl.when(c == 0)
                def _():
                    pltpu.make_async_copy(rep_hbm, field, rep_sem).wait()

            f, g = (c * size + offset for offset in PAIRS[name])
            acc[...] += one_frequency(f, 0) + one_frequency(g, 1)
            return
        which, starts = actions[name]
        arrived(c, which)
        start(c, *starts)

    for c in range(1, AHEAD):
        issue_zero(c)

    def steps(step, carry):
        @pl.when(step == 3)
        def _():
            pl.semaphore_wait(word.at[0], len(neighbours))
            greet(word.at[1])

        for name, lag in PROGRAM:
            c = step - lag
            if name == "send":
                pl.when(c < CHUNKS)(functools.partial(issue_zero, c))
            else:
                inside = jnp.logical_and(c >= 0, c < CHUNKS)
                pl.when(inside)(functools.partial(act, name, c))
        return carry

    lax.fori_loop(0, CHUNKS + max(lag for _, lag in PROGRAM), steps, 0)

    pl.semaphore_wait(word.at[1], len(neighbours))

    def spread(ref, me, peer, ssem, rsem):
        n = ref.shape[0]

        def one(step, carry):
            pltpu.make_async_remote_copy(
                src_ref=ref.at[me], dst_ref=ref.at[me], send_sem=ssem, recv_sem=rsem,
                device_id=peer(step), device_id_type=MESH,
            ).start()
            return carry

        lax.fori_loop(1, n, one, 0)

    def all_but_one(ref, semaphore):
        part = ref.at[pl.ds(0, ref.shape[0] - 1)]
        pltpu.make_async_copy(part, part, semaphore).wait()

    total = 2.0 / (lax.axis_size("freq") * freqs)
    sums[me_sum] = jnp.sum(acc[...], axis=0, keepdims=True) * total
    spread(sums, me_sum, sum_peer, sum_sem.at[0], sum_sem.at[1])
    all_but_one(gathered, send_sem)
    all_but_one(sums, sum_sem.at[1])
    parts[me_part] = jnp.sum(sums[...], axis=0)
    spread(parts, me_part, part_peer, part_sem.at[0], part_sem.at[1])
    all_but_one(sums, sum_sem.at[0])
    all_but_one(parts, part_sem.at[1])
    ambiguity = parts[cell * Y_LOW] + parts[cell * Y_LOW + 1]
    everywhere = jnp.sum(parts[...].reshape(n_cell, Y_LOW, cells), axis=1)
    peak = jnp.max(jnp.max(everywhere, axis=0, keepdims=True), axis=1, keepdims=True)
    out_ref[0:1, :] = ambiguity
    out_ref[1:2, :] = ambiguity / jnp.maximum(peak, 1.0)
    all_but_one(parts, part_sem.at[0])


def shards(covariance, replica, transmission):
    freqs, _, rows, depth = covariance.shape
    cells = replica.shape[3]
    n_freq, n_cell = lax.axis_size("freq"), lax.axis_size("cell")
    out = pl.pallas_call(
        kernel,
        out_shape=jax.ShapeDtypeStruct((2, cells), jnp.float32),
        in_specs=[pl.BlockSpec(memory_space=pltpu.HBM)] * 3,
        out_specs=pl.BlockSpec(memory_space=pltpu.VMEM),
        scratch_shapes=[
            pltpu.VMEM((freqs, 2, rows, depth // 2), jnp.bfloat16),
            pltpu.VMEM((freqs, rows, depth // 2), jnp.bfloat16),
            pltpu.VMEM((n_cell, freqs * 4, rows // 2, depth // 2), jnp.bfloat16),
            pltpu.VMEM((freqs, 2, depth, cells), jnp.bfloat16),
            pltpu.VMEM((freqs, cells), jnp.bfloat16),
            pltpu.VMEM((freqs, cells), jnp.float32),
            pltpu.VMEM((2, 2 * depth, 2 * depth), jnp.bfloat16),
            pltpu.VMEM((8, cells), jnp.float32),
            pltpu.VMEM((n_freq // Y_LOW, 1, cells), jnp.float32),
            pltpu.VMEM((n_cell * Y_LOW, 1, cells), jnp.float32),
            pltpu.SemaphoreType.DMA((5,)),
            pltpu.SemaphoreType.DMA,
            pltpu.SemaphoreType.DMA,
            pltpu.SemaphoreType.DMA((CHUNKS, GROUPS)),
            pltpu.SemaphoreType.DMA((2,)),
            pltpu.SemaphoreType.DMA((2,)),
            pltpu.SemaphoreType.REGULAR((2,)),
        ],
        compiler_params=pltpu.CompilerParams(collective_id=0, has_side_effects=True, vmem_limit_bytes=40 * 2**20),
    )(*[pltpu.with_memory_space_constraint(a, pltpu.HBM) for a in (covariance, replica, transmission)])
    return out[0], out[1]


def solution(mesh):
    return jax.shard_map(
        shards,
        mesh=mesh,
        in_specs=(P("freq", None, "cell", None), P("freq", None, None, "cell"), P("freq", "cell")),
        out_specs=(P("cell"), P("cell")),
        check_vma=False,
    )
```

```python
import functools

import jax
import jax.numpy as jnp
from jax import lax
from jax.experimental import pallas as pl
from jax.experimental.pallas import tpu as pltpu
from jax.sharding import PartitionSpec as P

MESH = pl.DeviceIdType.MESH
CHUNKS = 8
PIECES = 16
BY_X = 8
AHEAD = 4
PROGRAM = (
    ("over", 0),
    ("other", 2),
    ("x", 4),
    ("cx", 4),
    ("far", 2),
    ("near", 0),
    ("send", -AHEAD),
    ("y", 5),
    ("cy", 5),
)
PAIRS = {"cx": (0, 1), "cy": (2, 3)}
FIRST = "cx"
GROUPS = 6
CORES, Y_LOW = 2, 2


def kernel(
    cov_hbm, rep_hbm, trans_hbm, out_ref,
    diag, far, gathered, field, trans, weight, matrix, acc, sums, parts,
    load_sem, rep_sem, send_sem, recv_sem, sum_sem, part_sem, word,
):
    freq, cell = lax.axis_index("freq"), lax.axis_index("cell")
    n_cell = lax.axis_size("cell")
    ring = n_cell // 2
    x, row = lax.rem(cell, ring), lax.div(cell, ring)

    def at(shift, other=False):
        r = 1 - row if other else row
        return r * ring + lax.rem(x + shift + ring, ring)

    core, y_low = lax.rem(freq, CORES), lax.rem(lax.div(freq, CORES), Y_LOW)
    z = lax.div(freq, CORES * Y_LOW)
    me_sum, n_sum = z * CORES + core, sums.shape[0]
    me_part, n_part = cell * Y_LOW + y_low, parts.shape[0]

    def sum_peer(step):
        j = lax.rem(me_sum + step, n_sum)
        return {"freq": (lax.div(j, CORES) * Y_LOW + y_low) * CORES + lax.rem(j, CORES)}

    def part_peer(step):
        j = lax.rem(me_part + step, n_part)
        return {
            "freq": (z * Y_LOW + lax.rem(j, Y_LOW)) * CORES + core, "cell": lax.div(j, Y_LOW)
        }

    barrier = pltpu.get_barrier_semaphore()

    n_z = n_sum // CORES
    freq_at = lambda zz, yy, cc: {"freq": (zz * Y_LOW + yy) * CORES + cc}
    neighbours = (
        {"cell": at(1)}, {"cell": at(-1)}, {"cell": at(0, True)},
        freq_at(z, y_low, 1 - core),
        freq_at(lax.rem(z + 1, n_z), y_low, core), freq_at(lax.rem(z + n_z - 1, n_z), y_low, core),
        freq_at(z, 1 - y_low, core),
        {**freq_at(z, 1 - y_low, core), "cell": at(0, True)},
    )

    def greet(semaphore):
        for target in neighbours:
            pl.semaphore_signal(semaphore, inc=1, device_id=target, device_id_type=MESH)

    greet(barrier)

    def slot(shift, other=False):
        r, to = 1 - row if other else row, lax.rem(x + shift + ring, ring)
        return r * ring + lax.rem(to, 2) * (ring // 2) + lax.div(to, 2)

    beside = row * ring + (1 - lax.rem(x, 2)) * (ring // 2)

    lanes = gathered.shape[-1]
    freqs = field.shape[0]
    per_freq = gathered.shape[1] // freqs
    size = freqs // CHUNKS
    own = pl.ds(pl.multiple_of(row * lanes, lanes), lanes)
    other = pl.ds(pl.multiple_of((1 - row) * lanes, lanes), lanes)
    row_loads = []
    for i, part in enumerate((pl.ds(0, size), pl.ds(size, freqs - size))):
        row_loads.append((
            pltpu.make_async_copy(cov_hbm.at[part, :, :, own], diag.at[part], load_sem.at[2 * i]),
            pltpu.make_async_copy(
                cov_hbm.at[part, row, :, other], far.at[part], load_sem.at[2 * i + 1]
            ),
        ))
        for copy in row_loads[-1]:
            copy.start()
    trans_load = pltpu.make_async_copy(trans_hbm, trans, load_sem.at[4])
    trans_load.start()

    def load(c):
        part = pl.ds(c * size, size)
        return pltpu.make_async_copy(rep_hbm.at[part], field.at[part], rep_sem)

    def load_one(c, carry):
        load(c).start()
        return carry

    lax.fori_loop(0, CHUNKS, load_one, 0)

    shape = diag.shape[2:]
    rows = shape[0] // 2
    line = lax.broadcasted_iota(jnp.int32, shape, 0) + x * shape[0]
    column = lax.broadcasted_iota(jnp.int32, shape, 1)
    factor = jnp.where(line == column, 0.5, 1.0).astype(jnp.bfloat16)
    above = line <= column

    def pack(f, carry):
        packed = jnp.where(above, diag[f, 0] * factor, diag[f, 1])
        across = far[f]
        for i in range(2):
            gathered[slot(0), per_freq * f + i] = packed[i * rows:(i + 1) * rows]
            gathered[slot(0), per_freq * f + 2 + i] = across[i * rows:(i + 1) * rows]
        return carry

    for copy in row_loads[0]:
        copy.wait()
    lax.fori_loop(0, size, pack, 0, unroll=4)

    right, left, partner = at(1), at(-1), at(0, True)
    TO_PARTNER, TO_RIGHT, TO_LEFT, ON_RIGHT, ON_LEFT, BOTH_OVER = range(6)
    OTHER_RIGHT, OTHER_LEFT, FAR_OVER, OTHER_ON_RIGHT, OTHER_ON_LEFT = range(6, 11)
    NEAR, OVER, ON, OTHER, BY_Y, LAST = range(GROUPS)
    mid, mid_x, by_y = PIECES // 2, BY_X // 2, PIECES - BY_X
    table = {
        TO_PARTNER: (slot(0), partner, 0, PIECES, OVER),
        TO_RIGHT: (slot(0), right, 0, PIECES, NEAR),
        TO_LEFT: (slot(0), left, 0, PIECES, NEAR),
        ON_RIGHT: (slot(-1), right, 0, mid, ON),
        ON_LEFT: (slot(1), left, mid, PIECES - mid, ON),
        BOTH_OVER: (pl.ds(beside, 2), partner, BY_X, by_y, BY_Y),
        OTHER_RIGHT: (slot(0, True), right, 0, BY_X, OTHER),
        OTHER_LEFT: (slot(0, True), left, 0, BY_X, OTHER),
        FAR_OVER: (slot(2), partner, BY_X, by_y, BY_Y),
        OTHER_ON_RIGHT: (slot(-1, True), right, 0, mid_x, LAST),
        OTHER_ON_LEFT: (slot(1, True), left, mid_x, BY_X - mid_x, LAST),
    }
    landing = {
        NEAR: (pl.ds(0, 2), 0, PIECES),
        OVER: (slot(0, True), 0, PIECES),
        ON: (slot(2), 0, PIECES),
        OTHER: (pl.ds(0, 2), 0, BY_X),
        BY_Y: (pl.ds(0, 3), BY_X, by_y),
        LAST: (slot(2, True), 0, BY_X),
    }

    def start(c, *wanted):
        for kind in wanted:
            source, target, first, count, group = table[kind]
            ref = gathered.at[source, pl.ds(c * PIECES + first, count)]
            pltpu.make_async_remote_copy(
                src_ref=ref, dst_ref=ref,
                send_sem=send_sem, recv_sem=recv_sem.at[c, group],
                device_id={"cell": target}, device_id_type=MESH,
            ).start()

    def arrived(c, which):
        source, first, count = landing[which]
        ref = gathered.at[source, pl.ds(c * PIECES + first, count)]
        pltpu.make_async_copy(ref, ref, recv_sem.at[c, which]).wait()

    def issue_zero(c):
        start(c, TO_PARTNER, TO_RIGHT, TO_LEFT)

    actions = {
        "near": (NEAR, (ON_RIGHT, ON_LEFT, BOTH_OVER)),
        "over": (OVER, (OTHER_RIGHT, OTHER_LEFT)),
        "far": (ON, (FAR_OVER,)),
        "other": (OTHER, (OTHER_ON_RIGHT, OTHER_ON_LEFT)),
        "y": (BY_Y, ()),
        "x": (LAST, ()),
    }

    pl.semaphore_wait(barrier, len(neighbours))
    issue_zero(0)
    greet(word.at[0])
    for copy in row_loads[1]:
        copy.wait()
    lax.fori_loop(size, freqs, pack, 0, unroll=4)
    trans_load.wait()
    amplitude = trans[...].astype(jnp.float32)
    weight[...] = amplitude * amplitude
    acc[...] = jnp.zeros_like(acc)

    half = lanes
    tri_line = lax.broadcasted_iota(jnp.int32, (half, half), 0)
    tri_column = lax.broadcasted_iota(jnp.int32, (half, half), 1)
    upper = tri_line <= tri_column
    blank = jnp.zeros((half, half), jnp.bfloat16)
    depth2 = field.shape[1] * field.shape[2]
    cells = field.shape[3]

    def block(first, f, part):
        pieces = pl.ds(per_freq * f + 2 * part, 2)
        order = [first + to % 2 * (ring // 2) + to // 2 for to in range(ring)]
        return jnp.concatenate(
            [gathered[i, pieces].reshape(half // ring, half) for i in order]
        )

    for slot in range(2):
        for i, j in ((0, 3), (1, 0), (2, 1), (3, 2)):
            matrix[slot, pl.ds(i * half, half), pl.ds(j * half, half)] = blank

    def one_frequency(f, slot):
        def put(i, j, value):
            matrix[slot, pl.ds(i * half, half), pl.ds(j * half, half)] = value

        for b in range(2):
            packed = block(b * ring, f, 0)
            sym = jnp.where(upper, packed, blank)
            skew = jnp.where(upper, blank, packed)
            put(b, b, sym)
            put(2 + b, 2 + b, sym)
            put(2 + b, b, skew)
            put(b, 2 + b, -skew)
        across = block(0, f, 1)
        put(0, 1, across)
        put(2, 3, across)
        below = block(ring, f, 1)
        put(3, 0, below)
        put(1, 2, -below)
        v = field[f].reshape(depth2, cells)
        image = jnp.dot(matrix[slot], v, preferred_element_type=jnp.float32)
        power = jnp.sum((v.astype(jnp.float32) * image).reshape(depth2 // 8, 8, cells), axis=0)
        return power * weight[pl.ds(f, 1), :]

    def act(name, c):
        if name in PAIRS:
            if name == FIRST:

                @pl.when(c == 0)
                def _():
                    pltpu.make_async_copy(rep_hbm, field, rep_sem).wait()

            f, g = (c * size + offset for offset in PAIRS[name])
            acc[...] += one_frequency(f, 0) + one_frequency(g, 1)
            return
        which, starts = actions[name]
        arrived(c, which)
        start(c, *starts)

    for c in range(1, AHEAD):
        issue_zero(c)

    def steps(step, carry):
        @pl.when(step == 3)
        def _():
            pl.semaphore_wait(word.at[0], len(neighbours))
            greet(word.at[1])

        for name, lag in PROGRAM:
            c = step - lag
            if name == "send":
                pl.when(c < CHUNKS)(functools.partial(issue_zero, c))
            else:
                inside = jnp.logical_and(c >= 0, c < CHUNKS)
                pl.when(inside)(functools.partial(act, name, c))
        return carry

    lax.fori_loop(0, CHUNKS + max(lag for _, lag in PROGRAM), steps, 0)

    pl.semaphore_wait(word.at[1], len(neighbours))

    def spread(ref, me, peer, ssem, rsem):
        n = ref.shape[0]

        def one(step, carry):
            pltpu.make_async_remote_copy(
                src_ref=ref.at[me], dst_ref=ref.at[me], send_sem=ssem, recv_sem=rsem,
                device_id=peer(step), device_id_type=MESH,
            ).start()
            return carry

        lax.fori_loop(1, n, one, 0)

    def all_but_one(ref, semaphore):
        part = ref.at[pl.ds(0, ref.shape[0] - 1)]
        pltpu.make_async_copy(part, part, semaphore).wait()

    total = 2.0 / (lax.axis_size("freq") * freqs)
    sums[me_sum] = jnp.sum(acc[...], axis=0, keepdims=True) * total
    spread(sums, me_sum, sum_peer, sum_sem.at[0], sum_sem.at[1])
    all_but_one(gathered, send_sem)
    all_but_one(sums, sum_sem.at[1])
    parts[me_part] = jnp.sum(sums[...], axis=0)
    spread(parts, me_part, part_peer, part_sem.at[0], part_sem.at[1])
    all_but_one(sums, sum_sem.at[0])
    all_but_one(parts, part_sem.at[1])
    ambiguity = parts[cell * Y_LOW] + parts[cell * Y_LOW + 1]
    everywhere = jnp.sum(parts[...].reshape(n_cell, Y_LOW, cells), axis=1)
    peak = jnp.max(jnp.max(everywhere, axis=0, keepdims=True), axis=1, keepdims=True)
    out_ref[0:1, :] = ambiguity
    out_ref[1:2, :] = ambiguity / jnp.maximum(peak, 1.0)
    all_but_one(parts, part_sem.at[0])


def shards(covariance, replica, transmission):
    freqs, _, rows, depth = covariance.shape
    cells = replica.shape[3]
    n_freq, n_cell = lax.axis_size("freq"), lax.axis_size("cell")
    out = pl.pallas_call(
        kernel,
        out_shape=jax.ShapeDtypeStruct((2, cells), jnp.float32),
        in_specs=[pl.BlockSpec(memory_space=pltpu.HBM)] * 3,
        out_specs=pl.BlockSpec(memory_space=pltpu.VMEM),
        scratch_shapes=[
            pltpu.VMEM((freqs, 2, rows, depth // 2), jnp.bfloat16),
            pltpu.VMEM((freqs, rows, depth // 2), jnp.bfloat16),
            pltpu.VMEM((n_cell, freqs * 4, rows // 2, depth // 2), jnp.bfloat16),
            pltpu.VMEM((freqs, 2, depth, cells), jnp.bfloat16),
            pltpu.VMEM((freqs, cells), jnp.bfloat16),
            pltpu.VMEM((freqs, cells), jnp.float32),
            pltpu.VMEM((2, 2 * depth, 2 * depth), jnp.bfloat16),
            pltpu.VMEM((8, cells), jnp.float32),
            pltpu.VMEM((n_freq // Y_LOW, 1, cells), jnp.float32),
            pltpu.VMEM((n_cell * Y_LOW, 1, cells), jnp.float32),
            pltpu.SemaphoreType.DMA((5,)),
            pltpu.SemaphoreType.DMA,
            pltpu.SemaphoreType.DMA,
            pltpu.SemaphoreType.DMA((CHUNKS, GROUPS)),
            pltpu.SemaphoreType.DMA((2,)),
            pltpu.SemaphoreType.DMA((2,)),
            pltpu.SemaphoreType.REGULAR((2,)),
        ],
        compiler_params=pltpu.CompilerParams(collective_id=0, has_side_effects=True, vmem_limit_bytes=40 * 2**20),
    )(*[pltpu.with_memory_space_constraint(a, pltpu.HBM) for a in (covariance, replica, transmission)])
    return out[0], out[1]


def solution(mesh):
    return jax.shard_map(
        shards,
        mesh=mesh,
        in_specs=(P("freq", None, "cell", None), P("freq", None, None, "cell"), P("freq", "cell")),
        out_specs=(P("cell"), P("cell")),
        check_vma=False,
    )
```
